32 devices in a mesh: nodes: 2 (over core), gx: 4 (over z), gy: 4 (over y, x).
Axes of the slice: x: 2, y: 2, z: 4, core: 2. Of those that a mesh axis runs over, the one named last changes fastest.
Arguments:
- field_modes: float32 [4, 9, 256, 512], P(None, None, 'gx', 'gy'), may hold values from -4 to 4, as said below
- node_points: float32 [768, 8], replicated, may hold values from -1 to 1
- quad_weight: float32 [768], replicated, may hold values from 0.5 to 2
- group_of: int32 [768], replicated, may hold values from 0 to 2, as said below
Outputs:
- mean_field: float32 [256, 512], P('gx', 'gy')
- variance_field: float32 [256, 512], P('gx', 'gy')
The draws below stay inside these ranges and needn't reach their ends.
Inputs may be any that keep to these rules, and one draw needn't show every extreme that they name: `group_of`: one of the two groups (which one varies) is given exactly 384 nodes, the other between 48 and 96; all other nodes hold 2. `field_modes`: diffusivity fields (index 3) give a diffusivity between 0.1 and 1.4 at every node point in range; the other fields lie within the range.
All inputs are finite; a program needn't handle non-finite values.
Results may differ from the reference program's by a relative error of at most 0.00021.
Values sent between devices are 32-bit elements; how exact they have to be, the bound alone decides.
A program may use at most 192 MiB of HBM per device.

```python
import math
import jax
import jax.numpy as jnp
from jax import lax

BUSY = 384
STEPS = 4
DIMS = 8
NODES = 768
NX = 256
NY = 512


def draw_group_of(key, part):
    key_busy = jax.random.fold_in(key, 11)
    key_light = jax.random.fold_in(key, 12)
    key_order = jax.random.fold_in(key, 13)
    busy_group = jax.random.randint(key_busy, (), 0, 2)
    light_count = jax.random.randint(key_light, (), BUSY // 8, BUSY // 4 + 1)
    ordering = jax.random.permutation(key_order, NODES)
    placed = jnp.argsort(ordering)
    labels = jnp.where(placed < BUSY, busy_group, jnp.where(placed < BUSY + light_count, 1 - busy_group, 2))
    return labels.astype(jnp.int32)


def draw_field_modes(key, part):
    keys = [jax.random.fold_in(key, 21 + number) for number in range(5)]
    shaped = (DIMS + 1, NX, NY)
    initial = jnp.clip(jax.random.normal(keys[0], shaped), -4.0, 4.0)
    speeds = jnp.clip(0.25 * jax.random.normal(keys[1], (2,) + shaped), -1.0, 1.0)
    diff_base = jax.random.uniform(keys[2], (1, NX, NY), minval=0.5, maxval=1.0)
    diff_modes = jax.random.uniform(keys[4], (DIMS, NX, NY), minval=-0.05, maxval=0.05)
    diffusion = jnp.concatenate([diff_base, diff_modes], axis=0)
    return jnp.stack([initial, speeds[0], speeds[1], diffusion]).astype(jnp.float32)


def setup_inputs(seed: int = 0) -> dict:
    splits = jax.random.split(jax.random.key(seed), 5)
    return {
        "field_modes": draw_field_modes(jax.random.fold_in(splits[4], 71), 0),
        "node_points": jnp.clip(jax.random.uniform(splits[1], (NODES, DIMS), jnp.float32, -1.0, 1.0), -1.0, 1.0),
        "quad_weight": jnp.clip(jnp.exp(jax.random.uniform(splits[2], (NODES,), jnp.float32, math.log(0.5), math.log(2.0))), 0.5, 2.0),
        "group_of": draw_group_of(jax.random.fold_in(splits[4], 71), 0),
    }


TIME_STEP = 0.15


def advance_cells(centre, east_side, west_side, north_side, south_side, x_speed, y_speed, diffusion):
    laplace = (east_side + west_side + north_side + south_side) - 4.0 * centre
    transport = x_speed * ((east_side - west_side) * 0.5) + y_speed * ((north_side - south_side) * 0.5)
    return centre + TIME_STEP * (diffusion * laplace - transport)


def evolve(coefficients, field_modes):
    params = jnp.einsum("bk,ckxy->bcxy", coefficients, field_modes, precision=lax.Precision.HIGHEST)
    state = params[:, 0]
    for section in range(STEPS):
        east_side = jnp.roll(state, -1, axis=1)
        west_side = jnp.roll(state, 1, axis=1)
        north_side = jnp.roll(state, -1, axis=2)
        south_side = jnp.roll(state, 1, axis=2)
        state = advance_cells(state, east_side, west_side, north_side, south_side, params[:, 1], params[:, 2], params[:, 3])
    return state


def reference(field_modes, node_points, quad_weight, group_of):
    included = (group_of < 2).astype(jnp.float32)
    weight = quad_weight * included
    weight_total = jnp.sum(weight)
    coefficients = jnp.concatenate([jnp.ones((NODES, 1), jnp.float32), node_points], axis=1)
    blocks = NODES // 16
    coeff_blocks = coefficients.reshape(blocks, 16, DIMS + 1)
    weight_blocks = weight.reshape(blocks, 16)

    def accumulate(carry, pieces):
        state = evolve(pieces[0], field_modes)
        first = carry[0] + jnp.einsum("b,bxy->xy", pieces[1], state, precision=lax.Precision.HIGHEST)
        second = carry[1] + jnp.einsum("b,bxy->xy", pieces[1], state * state, precision=lax.Precision.HIGHEST)
        return (first, second), None

    start = (jnp.zeros((NX, NY), jnp.float32), jnp.zeros((NX, NY), jnp.float32))
    (first, second), unused = lax.scan(accumulate, start, (coeff_blocks, weight_blocks))
    mean_field = first / weight_total
    variance_field = second / weight_total - mean_field * mean_field
    return mean_field, variance_field
```

```python
import functools

import jax
import jax.numpy as jnp
from jax import lax
from jax.experimental import pallas as pl
from jax.experimental.pallas import tpu as pltpu
from jax.sharding import PartitionSpec as P

STEPS = 4
TIME_STEP = 0.15
LANES = 128


def extended(x, axis, dim, width):
    size, length = lax.axis_size(axis), x.shape[dim]
    up = [(i, (i + 1) % size) for i in range(size)]
    down = [(j, i) for i, j in up]
    last = lax.slice_in_dim(x, length - width, length, axis=dim)
    initial = lax.slice_in_dim(x, 0, width, axis=dim)
    before = lax.ppermute(last, axis, up)
    after = lax.ppermute(initial, axis, down)
    return jnp.concatenate([before, x, after], axis=dim)


def split(x):
    high = lax.reduce_precision(x, 8, 7)
    return high.astype(jnp.bfloat16), (x - high).astype(jnp.bfloat16)


def kernel(rows, cols, field_ref, coef_ref, weight_ref, out_ref, ua, ub, bx, by, ka):
    wide = cols + 2 * STEPS
    tall = rows + 2 * STEPS
    blocks = wide // 8
    half = pl.program_id(0)

    @pl.when(half == 0)
    def _():
        out_ref[...] = jnp.zeros_like(out_ref)

    @pl.loop(0, tall)
    def _(x):
        here = pl.ds(pl.multiple_of(x * wide, 8), wide)
        made = jnp.dot(field_ref[here, :], coef_ref[0], preferred_element_type=jnp.float32)
        for n, ref in enumerate((ua, bx, by, ka)):
            ref[here, :] = made[:, n * LANES : (n + 1) * LANES]

    def advance(src, base):
        c = src[pl.ds(base, 8), :]
        e = src[pl.ds(base + wide, 8), :]
        w = src[pl.ds(base - wide, 8), :]
        n = src[pl.ds(base + 1, 8), :]
        s = src[pl.ds(base - 1, 8), :]
        at = pl.ds(base, 8)
        lap = ((e + w) + (n + s)) - 4.0 * c
        return c + ((ka[at, :] * lap - bx[at, :] * (e - w)) - by[at, :] * (n - s))

    for step in range(STEPS - 1):
        src, dst = (ua, ub) if step % 2 == 0 else (ub, ua)
        count = (tall - 2 * (step + 1)) // 2

        @pl.loop(0, count)
        def _(pair):
            start = (pair * 2 + step + 1) * wide
            for block in range(blocks):
                for r in range(2):
                    base = pl.multiple_of(start + r * wide + block * 8, 8)
                    dst[pl.ds(base, 8), :] = advance(src, base)

    src = ua if (STEPS - 1) % 2 == 0 else ub
    weight = weight_ref[0]
    lane = lax.broadcasted_iota(jnp.int32, (8, LANES), 1)
    sub = lax.broadcasted_iota(jnp.int32, (8, LANES), 0)

    @pl.loop(0, rows)
    def _(x):
        start = (x + STEPS) * wide
        first = jnp.zeros((8, LANES), jnp.float32)
        second = jnp.zeros((8, LANES), jnp.float32)
        for block in range(blocks):
            base = pl.multiple_of(start + block * 8, 8)
            u = advance(src, base)
            wu = weight * u
            f = jnp.sum(wu, axis=1, keepdims=True)
            g = jnp.sum(wu * u, axis=1, keepdims=True)
            hit = (lane + STEPS) == (sub + block * 8)
            first = jnp.where(hit, f, first)
            second = jnp.where(hit, g, second)
        out_ref[0, pl.ds(x, 1), :] += jnp.sum(first, axis=0, keepdims=True)
        out_ref[1, pl.ds(x, 1), :] += jnp.sum(second, axis=0, keepdims=True)


def on_device(field_modes, node_points, quad_weight, group_of):
    fields, modes, rows, cols = field_modes.shape
    nodes = group_of.shape[0]
    members = lax.axis_size("nodes")
    most = nodes // 2 + nodes // 8
    cap = -(-most // (members * LANES)) * LANES
    halves = cap // LANES
    member = lax.axis_index("nodes")
    chosen = group_of < 2
    rank = jnp.cumsum(chosen.astype(jnp.int32)) - 1 - member * cap
    target = jnp.arange(cap, dtype=jnp.int32)
    select = (chosen[None, :] & (rank[None, :] == target[:, None])).astype(jnp.float32)
    table = jnp.concatenate(
        [jnp.ones((nodes, 1), jnp.float32), node_points, quad_weight[:, None]], axis=1
    )
    picked = jnp.dot(select, table, precision=lax.Precision.HIGHEST)
    coef = picked[:, :modes].T
    weight = picked[:, modes].reshape(halves, 1, LANES)
    weight_total = jnp.sum(quad_weight * chosen.astype(jnp.float32))

    scale = jnp.array([1.0, 0.5 * TIME_STEP, 0.5 * TIME_STEP, TIME_STEP], jnp.float32)
    mixed = jnp.einsum("fo,jn->fjon", jnp.diag(scale), coef, precision=lax.Precision.HIGHEST)
    mixed = mixed.reshape(fields * modes, fields, halves, LANES)
    mixed = mixed.transpose(2, 0, 1, 3).reshape(halves, fields * modes, fields * LANES)
    c_high, c_low = split(mixed)
    depth = 3 * fields * modes
    pad = -depth % LANES
    stacked = jnp.pad(jnp.concatenate([c_high, c_high, c_low], axis=1), ((0, 0), (0, pad), (0, 0)))

    wide, tall = cols + 2 * STEPS, rows + 2 * STEPS
    field = field_modes.reshape(fields * modes, rows, cols)
    field = extended(field, "gx", 1, STEPS)
    field = extended(field, "gy", 2, STEPS)
    field = field.reshape(fields * modes, tall * wide)
    f_high, f_low = split(field)
    field = jnp.pad(jnp.concatenate([f_high, f_low, f_high], axis=0), ((0, pad), (0, 0))).T

    cells = tall * wide
    sums = pl.pallas_call(
        functools.partial(kernel, rows, cols),
        grid=(halves,),
        out_shape=jax.ShapeDtypeStruct((2, rows, cols), jnp.float32),
        in_specs=[
            pl.BlockSpec((cells, depth + pad), lambda h: (0, 0)),
            pl.BlockSpec((1, depth + pad, fields * LANES), lambda h: (h, 0, 0)),
            pl.BlockSpec((1, 1, LANES), lambda h: (h, 0, 0)),
        ],
        out_specs=pl.BlockSpec((2, rows, cols), lambda h: (0, 0, 0)),
        scratch_shapes=[pltpu.VMEM((cells, LANES), jnp.float32)] * 5,
    )(field, stacked, weight)
    swap = [(i, (i + 1) % members) for i in range(members)]
    part = sums
    for _ in range(members - 1):
        part = lax.ppermute(part, "nodes", swap)
        sums = sums + part
    mean_field = sums[0] / weight_total
    variance_field = sums[1] / weight_total - mean_field * mean_field
    return (mean_field, variance_field)


def solution(mesh):
    placed = (P(None, None, "gx", "gy"), P(), P(), P())
    return jax.shard_map(
        on_device,
        mesh=mesh,
        in_specs=placed,
        out_specs=(P("gx", "gy"), P("gx", "gy")),
        check_vma=False,
    )
```
